32 devices in a mesh: rep: 2 (over x), ep: 8 (over z, y), tp: 2 (over core).
Axes of the slice: x: 2, y: 2, z: 4, core: 2. Of those that a mesh axis runs over, the one named last changes fastest.
Arguments:
- tokens: bfloat16 [1024, 3072], P(('rep', 'ep')), parts along dimension 0, may hold values from -6 to 6
- routes: int32 [1024, 2], P(('rep', 'ep')), parts along dimension 0, may hold values from 0 to 3, all different within a row; in each aligned block of 64 rows (0 to 63, 64 to 127, ...) at most 40 rows name the same one
- route_weight: float32 [1024, 2], P(('rep', 'ep')), parts along dimension 0, may hold values from 0.2 to 1
- gate_code: bfloat16 [3072, 32768], P(None, ('ep', 'tp')), may hold values from -0.109375 to 0.109375
- gate_scale: float32 [3072, 256], P(None, ('ep', 'tp')), may hold values from 0.5 to 2
- up_code: bfloat16 [3072, 32768], P(None, ('ep', 'tp')), may hold values from -0.109375 to 0.109375
- up_scale: float32 [3072, 256], P(None, ('ep', 'tp')), may hold values from 0.5 to 2
- down_code: bfloat16 [32768, 3072], P(('ep', 'tp')), may hold values from -0.0625 to 0.0625
- down_scale: float32 [32768, 24], P(('ep', 'tp')), may hold values from 0.5 to 2
Outputs:
- mixed: bfloat16 [1024, 3072], P(('rep', 'ep'), 'tp'), parts along dimension 0
The draws below stay inside these ranges and needn't reach their ends.
There are 2 independent parts, one for each index of `rep`. The reference program is written for one: setup_inputs(seed, part) draws one part's arguments, and reference() takes and returns one part's arrays. A program takes and returns all parts, laid end to end along the dimension named above; an argument that names none is the same for every part. Nothing has to cross between parts.
Inputs may be any that keep to these rules, and one draw needn't show every extreme that they name: `routes`: among the 64 rows of one index of ep, no expert is named by more than 40 rows, a bound that some block reaches; a row names 2 different experts.
All inputs are finite; a program needn't handle non-finite values.
Results may differ from the reference program's by a relative error of at most 0.02.
Values may be sent and summed in bfloat16 or wider, within the bound.
No kernel may reach another device: no remote copies, remote signals or barrier semaphores. Data moves between devices by JAX's collectives and lax.ppermute only.
A program may use at most 128 MiB of HBM per device.

```python
import math
import jax
import jax.numpy as jnp
import numpy as np
from jax import lax

D = 3072
FF = 8192
EXPERTS = 4
TOP = 2
QB = 128
TOK_DEV = 64
CAP = 40
TOKENS = 512
N_EP = 8


def levels(rng, shape, pieces, least, top_value):
    loudness = 1.0
    for axis_at, blocks in pieces:
        heights = jax.random.uniform(jax.random.fold_in(jax.random.fold_in(rng, 6), axis_at), (blocks,), jnp.float32, least / len(pieces), top_value / len(pieces))
        loudness = loudness * jnp.repeat(jnp.exp(heights), shape[axis_at] // blocks).reshape((-1,) + (1,) * (len(shape) - 1 - axis_at))
    return loudness


def deal_out(own_key, own, number, rows, count, top, bound, skew):
    order = jax.random.permutation(own_key, count)
    crowded, usual = load_shares(count, rows * top, bound, skew, True), load_shares(count, rows * top, bound, skew, False)
    places = jnp.arange(count)

    def named(sizes, turn):
        used = int((sizes > 0).sum())
        fixed = max(1, used // 4)
        moved = fixed + (places - fixed + turn * (used - fixed)) % max(1, count - fixed)
        return jnp.zeros((count,), jnp.int32).at[order[jnp.where(places < fixed, places, moved)]].set(jnp.asarray(sizes, jnp.int32))

    sizes = jnp.where(number % 4 == 0, named(crowded, number // 4), named(usual, number - number // 4 - 1))
    mixed = jax.random.permutation(jax.random.fold_in(own, 3), count)
    giver, receiver = mixed[0:count // 2 * 2:2], mixed[1:count // 2 * 2:2]
    slack = jnp.minimum(sizes[giver] - 1, bound - sizes[receiver]) // 2
    slack = jnp.where((giver == order[0]) | (receiver == order[0]) | (sizes[receiver] == 0), 0, jnp.maximum(slack, 0))
    moved = jax.random.randint(jax.random.fold_in(own, 4), (count // 2,), 0, 1 << 20) % (slack + 1)
    sizes = sizes.at[giver].add(-moved).at[receiver].add(moved)
    labels = jnp.searchsorted(jnp.cumsum(sizes), jnp.arange(rows * top), side="right").astype(jnp.int32)
    listing = labels.reshape(top, rows).T
    listing = listing[jax.random.permutation(jax.random.fold_in(own, 1), rows)]
    turn = jax.random.randint(jax.random.fold_in(own, 2), (rows, 1), 0, top)
    return jnp.take_along_axis(listing, (jnp.arange(top)[None, :] + turn) % top, axis=1)


def load_shares(count, total, limit, lean, full):
    loads = [(1 << 20) // math.isqrt(standing ** lean) + 1 for standing in range(1, count + 1)]
    largest = limit if full else min(limit, max(-(-total // count), total * loads[0] // sum(loads)))
    least = 1 if total - largest >= count - 1 else 0
    given, surplus = [largest] + [least] * (count - 1), total - largest - least * (count - 1)
    while surplus > 0:
        movable = [i for i in range(1, count) if given[i] < largest] or [i for i in range(1, count) if given[i] < limit]
        pool, left = sum([loads[i] for i in movable]), surplus
        for i in movable:
            extra = min(limit - given[i], max(1, left * loads[i] // pool), surplus)
            given[i] = given[i] + extra
            surplus = surplus - extra
    return np.array(given)


def scatter_about(key, shape, width, limit, shards=(), held_as=jnp.bfloat16):
    level = levels(key, shape, shards, -0.22, 0.18) if shards else 1.0
    values = jax.random.normal(key, shape, jnp.float32) * width * level
    return jnp.minimum(jnp.maximum(values, -limit), limit).astype(held_as)


def setup_inputs(seed: int = 0, part: int = 0) -> dict:
    key_of = jax.random.split(jax.random.key(seed), 10)
    part_keys = jax.random.split(jax.random.fold_in(key_of[9], part), 10)
    tokens = scatter_about(part_keys[0], (TOKENS, D), 1.0, 6.0, ((0, 8),))
    routes_keys = jax.random.split(jax.random.fold_in(part_keys[1], 1), TOKENS // TOK_DEV)
    routes_turns = jax.random.permutation(jax.random.fold_in(part_keys[1], 3), TOKENS // TOK_DEV)
    routes = jax.vmap(lambda own, number: deal_out(jax.random.fold_in(part_keys[1], 2), own, number, TOK_DEV, EXPERTS, TOP, CAP, 2))(routes_keys, routes_turns).reshape((TOKENS, TOP))
    route_weight = jnp.clip(0.2 + 0.8 * jax.random.uniform(part_keys[2], (TOKENS, TOP), jnp.float32) ** levels(part_keys[2], (TOKENS, TOP), ((0, 8),), -0.2, 0.2), 0.2, 1.0)
    gate_code = scatter_about(key_of[3], (D, EXPERTS * FF), D ** -0.5, 0.109375, ((1, 16),))
    gate_scale = jnp.clip(jnp.exp(math.log(2.0) - 1.3862944 * jax.random.uniform(key_of[4], (D, EXPERTS * FF // QB), jnp.float32) ** levels(key_of[4], (D, EXPERTS * FF // QB), ((1, 16),), -0.2, 0.2)), 0.5, 2.0)
    up_code = scatter_about(key_of[5], (D, EXPERTS * FF), D ** -0.5, 0.109375, ((1, 16),))
    up_scale = jnp.clip(jnp.exp(math.log(2.0) - 1.3862944 * jax.random.uniform(key_of[6], (D, EXPERTS * FF // QB), jnp.float32) ** levels(key_of[6], (D, EXPERTS * FF // QB), ((1, 16),), -0.2, 0.2)), 0.5, 2.0)
    down_code = scatter_about(key_of[7], (EXPERTS * FF, D), FF ** -0.5, 0.0625, ((0, 16),))
    down_scale = jnp.clip(jnp.exp(math.log(2.0) - 1.3862944 * jax.random.uniform(key_of[8], (EXPERTS * FF, D // QB), jnp.float32) ** levels(key_of[8], (EXPERTS * FF, D // QB), ((0, 16),), -0.2, 0.2)), 0.5, 2.0)
    return dict(tokens=tokens, routes=routes, route_weight=route_weight, gate_code=gate_code, gate_scale=gate_scale, up_code=up_code, up_scale=up_scale, down_code=down_code, down_scale=down_scale)


def dequant(code, scale):
    return (code.astype(jnp.float32) * jnp.repeat(scale, QB, axis=1)).astype(jnp.bfloat16)


def slot_table(expert_ids):
    onehot = (expert_ids[:, None] == jnp.arange(EXPERTS, dtype=jnp.int32)[None, :]).astype(jnp.int32)
    before = jnp.cumsum(onehot, axis=0) - onehot
    return jnp.sum(before * onehot, axis=1).astype(jnp.int32)


def reference(tokens, routes, route_weight, gate_code, gate_scale, up_code, up_scale, down_code, down_scale):
    token_blocks = tokens.reshape(N_EP, TOK_DEV, D)
    expert_ids = routes.reshape(N_EP, TOK_DEV * TOP)
    pair_weight = route_weight.reshape(N_EP, TOK_DEV * TOP)
    slot_rank = jax.vmap(slot_table)(expert_ids)
    target = expert_ids * CAP + slot_rank
    columns = jnp.arange(EXPERTS * CAP, dtype=jnp.int32)
    picked = (target[:, None, :] == columns[None, :, None]).astype(jnp.float32)
    repeated = jnp.repeat(token_blocks, TOP, axis=1).astype(jnp.float32)
    buffers = jnp.einsum("scp,spd->scd", picked, repeated).astype(jnp.bfloat16)
    buffers = buffers.reshape(N_EP, EXPERTS, CAP, D)
    outputs = []
    for expert in range(EXPERTS):
        low = expert * FF
        w_gate = dequant(gate_code[:, low:low + FF], gate_scale[:, low // QB:(low + FF) // QB])
        w_up = dequant(up_code[:, low:low + FF], up_scale[:, low // QB:(low + FF) // QB])
        w_down = dequant(down_code[low:low + FF, :], down_scale[low:low + FF, :])
        expert_rows = buffers[:, expert].reshape(N_EP * CAP, D)
        gate_act = jnp.dot(expert_rows, w_gate, preferred_element_type=jnp.float32)
        up_act = jnp.dot(expert_rows, w_up, preferred_element_type=jnp.float32)
        hidden = (jax.nn.silu(gate_act) * up_act).astype(jnp.bfloat16)
        result = jnp.dot(hidden, w_down, preferred_element_type=jnp.float32)
        outputs.append(result.reshape(N_EP, CAP, D))
    stacked = jnp.stack(outputs, axis=1).reshape(N_EP, EXPERTS * CAP, D)
    mixing = jnp.where(target[:, :, None] == columns[None, None, :], pair_weight[:, :, None], 0.0)
    mixing = mixing.astype(jnp.float32).reshape(N_EP, TOK_DEV, TOP, EXPERTS * CAP).sum(axis=2)
    mixed = jnp.einsum("spc,scd->spd", mixing, stacked, precision=lax.Precision.HIGHEST)
    return mixed.reshape(TOKENS, D).astype(jnp.bfloat16)
```

```python
import functools

import jax
import jax.numpy as jnp
from jax import lax
from jax.experimental import pallas as pl
from jax.experimental.pallas import tpu as pltpu
from jax.sharding import PartitionSpec as P

EXPERTS = 4
TOP = 2
QB = 128
CAP = 40
F32 = jnp.float32
BF16 = jnp.bfloat16
VMEM = pltpu.VMEM
MIB = 2**20


def whole():
    return pl.BlockSpec(memory_space=VMEM)


def scalar():
    return pl.BlockSpec(memory_space=pltpu.SMEM)


def ranks(routes_t, expert):
    count = routes_t.shape[1]
    named = (routes_t[0:1, :] == expert).astype(F32)
    for k in range(1, TOP):
        named = named + (routes_t[k : k + 1, :] == expert).astype(F32)
    rows = lax.broadcasted_iota(jnp.int32, (count, count), 0)
    cols = lax.broadcasted_iota(jnp.int32, (count, count), 1)
    earlier = (rows < cols).astype(F32)
    wide = jnp.broadcast_to(named, (8, count))
    return named, jnp.dot(wide, earlier, preferred_element_type=F32)[0:1, :]


def pack_kernel(place, routes_ref, tokens_ref, *outs):
    own = place[0]
    routes_t = routes_ref[...]
    count = routes_t.shape[1]
    slots = lax.broadcasted_iota(jnp.int32, (CAP, count), 0)
    for d, out in enumerate(outs):
        named, rank = ranks(routes_t, own ^ d)
        hit = (slots == rank.astype(jnp.int32)) & (jnp.broadcast_to(named, (CAP, count)) > 0.5)
        picked = jnp.where(hit, 1.0, 0.0).astype(BF16)
        out[...] = jnp.dot(picked, tokens_ref[...], preferred_element_type=F32).astype(BF16)


def pack(place, routes_t, tokens, parts):
    count, width = tokens.shape
    part = width // parts
    return pl.pallas_call(
        pack_kernel,
        grid_spec=pltpu.PrefetchScalarGridSpec(
            num_scalar_prefetch=1,
            grid=(1,),
            in_specs=[
                pl.BlockSpec(routes_t.shape, lambda i, place: (0, 0)),
                pl.BlockSpec((count, part), lambda i, place: (0, place[1])),
            ],
            out_specs=[pl.BlockSpec((CAP, part), lambda i, place: (0, 0))] * EXPERTS,
        ),
        out_shape=[jax.ShapeDtypeStruct((CAP, part), BF16)] * EXPERTS,
        compiler_params=pltpu.CompilerParams(vmem_limit_bytes=4 * MIB),
        name="pack",
    )(place, routes_t, tokens)


def dequant_kernel(code, scale_t, out):
    rows = code.shape[0]
    start = pl.multiple_of(pl.program_id(0) * rows, rows)
    scale = scale_t[...].T
    for b in range(code.shape[1] // QB):
        cols = slice(b * QB, (b + 1) * QB)
        out[pl.ds(start, rows), cols] = (code[:, cols].astype(F32) * scale[:, b : b + 1]).astype(BF16)


def dequant(code, scale_t, name):
    rows, width = code.shape
    step = min(256, rows)
    code = pltpu.with_memory_space_constraint(code, pltpu.HBM)
    return pl.pallas_call(
        dequant_kernel,
        grid=(rows // step,),
        in_specs=[
            pl.BlockSpec((step, width), lambda i: (i, 0)),
            pl.BlockSpec((scale_t.shape[0], step), lambda i: (0, i)),
        ],
        out_specs=whole(),
        out_shape=VMEM((rows, width), BF16),
        compiler_params=pltpu.CompilerParams(vmem_limit_bytes=8 * MIB),
        cost_estimate=pl.CostEstimate(flops=4 * 10**9, bytes_accessed=2 * rows * width, transcendentals=0),
        name=name,
    )(code, scale_t)


def hidden_kernel(parts, place, *refs):
    xs, (w_gate, w_up, out) = refs[:parts], refs[parts:]
    part = xs[0].shape[1]
    block = min(256, out.shape[1])
    for n in range(out.shape[1] // block):
        cols = slice(n * block, (n + 1) * block)
        gate = up = None
        for p, x in enumerate(xs):
            at = pl.ds(pl.multiple_of(lax.rem(place[1] + p, parts) * part, part), part)
            g = jnp.dot(x[...], w_gate[at, cols], preferred_element_type=F32)
            u = jnp.dot(x[...], w_up[at, cols], preferred_element_type=F32)
            gate = g if gate is None else gate + g
            up = u if up is None else up + u
        out[:, cols] = (gate / (1.0 + jnp.exp(-gate)) * up).astype(BF16)


def hidden_of(place, xs, w_gate, w_up, name):
    rows = xs[0].shape[0]
    width = w_gate.shape[1]
    flops = 4 * rows * w_gate.shape[0] * width
    return pl.pallas_call(
        functools.partial(hidden_kernel, len(xs)),
        in_specs=[scalar()] + [whole()] * (len(xs) + 2),
        out_specs=whole(),
        out_shape=VMEM((rows, width), BF16),
        compiler_params=pltpu.CompilerParams(vmem_limit_bytes=8 * MIB),
        cost_estimate=pl.CostEstimate(flops=flops, bytes_accessed=0, transcendentals=rows * width),
        name=name,
    )(place, *xs, w_gate, w_up)


def down_kernel(count, shift, parts, place, *refs):
    hs, w, outs = refs[:count], refs[count], refs[count + 1 :]
    part = outs[0].shape[1]
    block = min(256, part)
    base = lax.rem(place[1] + shift, parts) * part
    for h, out in zip(hs, outs):
        for n in range(part // block):
            at = pl.ds(pl.multiple_of(base + n * block, block), block)
            out[:, n * block : (n + 1) * block] = jnp.dot(
                h[...], w[:, at], preferred_element_type=F32
            ).astype(out.dtype)


def down(place, hs, w, shift, parts, dtype, name):
    part = w.shape[1] // parts
    rows = sum(h.shape[0] for h in hs)
    return pl.pallas_call(
        functools.partial(down_kernel, len(hs), shift, parts),
        in_specs=[scalar()] + [whole()] * (len(hs) + 1),
        out_specs=[whole()] * len(hs),
        out_shape=[VMEM((h.shape[0], part), dtype) for h in hs],
        compiler_params=pltpu.CompilerParams(vmem_limit_bytes=8 * MIB),
        cost_estimate=pl.CostEstimate(flops=2 * rows * w.shape[0] * part, bytes_accessed=0, transcendentals=0),
        name=name,
    )(place, *hs, w)


def mix_kernel(place, routes_ref, weight_ref, *refs):
    pieces, out = refs[:-1], refs[-1]
    own = place[0]
    routes_t = routes_ref[...]
    count = routes_t.shape[1]
    weight = weight_ref[...].T
    slots = lax.broadcasted_iota(jnp.int32, (CAP, TOP * count), 0)
    both = jnp.concatenate([routes_t[k : k + 1, :] for k in range(TOP)], axis=1)
    gathered = None
    for d, piece in enumerate(pieces):
        expert = own ^ d
        _, rank = ranks(routes_t, expert)
        wide = jnp.concatenate([rank] * TOP, axis=1).astype(jnp.int32)
        hit = (slots == wide) & (jnp.broadcast_to(both, slots.shape) == expert)
        picked = jnp.where(hit, 1.0, 0.0).astype(BF16)
        got = lax.dot_general(
            picked, piece[...], (((0,), (0,)), ((), ())), preferred_element_type=F32
        )
        gathered = got if gathered is None else gathered + got
    total = None
    for k in range(TOP):
        term = gathered[k * count : (k + 1) * count, :] * weight[:, k : k + 1]
        total = term if total is None else total + term
    out[...] = total.astype(BF16)


def mix(place, routes_t, weight_t, pieces):
    count = routes_t.shape[1]
    part = pieces[0].shape[1]
    return pl.pallas_call(
        mix_kernel,
        in_specs=[scalar()] + [whole()] * (2 + len(pieces)),
        out_specs=whole(),
        out_shape=jax.ShapeDtypeStruct((count, part), BF16),
        compiler_params=pltpu.CompilerParams(vmem_limit_bytes=8 * MIB),
        name="mix",
    )(place, routes_t, weight_t, *pieces)


def layer(
    members, parts, tokens, routes, route_weight,
    gate_code, gate_scale, up_code, up_scale, down_code, down_scale,
):
    def send(x, where):
        pairs = []
        for e in range(EXPERTS):
            for m in range(members):
                for t in range(parts):
                    e2, m2, t2 = where(e, m, t)
                    pairs.append(((e * members + m) * parts + t, (e2 * members + m2) * parts + t2))
        return lax.ppermute(x, ("ep", "tp"), pairs)

    def to_expert(x, d):
        return x if d == 0 else send(x, lambda e, m, t: (e ^ d, m, t))

    def to_member(x, s):
        return x if s == 0 else send(x, lambda e, m, t: (e, (m + s) % members, t))

    def to_part(x, p):
        return x if p == 0 else send(x, lambda e, m, t: (e, m, (t + p) % parts))

    place = jnp.stack([lax.axis_index("ep") // members, lax.axis_index("tp")]).astype(jnp.int32)
    routes_t, weight_t = routes.T, route_weight.T
    order = list(range(EXPERTS))
    far_first = sorted(order, reverse=True)

    outgoing = pack(place, routes_t, tokens, parts)
    arrived = {d: to_expert(outgoing[d], d) for d in far_first}
    shared = {(s, d): to_member(arrived[d], s) for s in range(members) for d in order}
    w_gate = dequant(gate_code, gate_scale.T, "dequant_gate")
    w_up = dequant(up_code, up_scale.T, "dequant_up")
    w_down = dequant(down_code, down_scale.T, "dequant_down")
    hiddens = []
    for s in range(members):
        own = jnp.concatenate([shared[s, d] for d in order], axis=0)
        xs = [to_part(own, (parts - p) % parts) for p in range(parts)]
        hiddens.append(hidden_of(place, xs, w_gate, w_up, f"hidden_{s}"))
    sums = None
    for p in range(1, parts):
        partial = down(place, hiddens, w_down, p, parts, BF16, f"down_{p}")
        partial = [to_part(x, p) for x in partial]
        sums = partial if sums is None else [a.astype(F32) + b.astype(F32) for a, b in zip(sums, partial)]
    own = down(place, hiddens, w_down, 0, parts, F32, "down_0")
    sums = own if sums is None else [a + b.astype(F32) for a, b in zip(own, sums)]

    def rows_of(x, d):
        return lax.slice_in_dim(x, d * CAP, (d + 1) * CAP, axis=0)

    pieces = {}
    for d in far_first:
        total = rows_of(sums[0], d)
        for s in range(1, members):
            back = to_member(rows_of(sums[s], d).astype(BF16), members - s)
            total = total + back.astype(F32)
        pieces[d] = to_expert(total.astype(BF16), d)
    return mix(place, routes_t, weight_t, [pieces[d] for d in order])


def solution(mesh):
    members = mesh.shape["ep"] // EXPERTS
    parts = mesh.shape["tp"]
    rows = P(("rep", "ep"), None)
    columns = P(None, ("ep", "tp"))
    placed = (rows, rows, rows, columns, columns, columns, columns, P(("ep", "tp"), None), P(("ep", "tp"), None))
    return jax.shard_map(
        functools.partial(layer, members, parts),
        mesh=mesh,
        in_specs=placed,
        out_specs=P(("rep", "ep"), "tp"),
        check_vma=False,
    )
```

```python
import functools

import jax
import jax.numpy as jnp
from jax import lax
from jax.experimental import pallas as pl
from jax.experimental.pallas import tpu as pltpu
from jax.sharding import PartitionSpec as P

EXPERTS = 4
TOP = 2
QB = 128
CAP = 40
F32 = jnp.float32
BF16 = jnp.bfloat16
VMEM = pltpu.VMEM
MIB = 2**20


def whole():
    return pl.BlockSpec(memory_space=VMEM)


def scalar():
    return pl.BlockSpec(memory_space=pltpu.SMEM)


def ranks(routes_t, expert):
    count = routes_t.shape[1]
    named = (routes_t[0:1, :] == expert).astype(F32)
    for k in range(1, TOP):
        named = named + (routes_t[k : k + 1, :] == expert).astype(F32)
    rows = lax.broadcasted_iota(jnp.int32, (count, count), 0)
    cols = lax.broadcasted_iota(jnp.int32, (count, count), 1)
    earlier = (rows < cols).astype(F32)
    wide = jnp.broadcast_to(named, (8, count))
    return named, jnp.dot(wide, earlier, preferred_element_type=F32)[0:1, :]


def pack_kernel(place, routes_ref, tokens_ref, *outs):
    own = place[0]
    routes_t = routes_ref[...]
    count = routes_t.shape[1]
    slots = lax.broadcasted_iota(jnp.int32, (CAP, count), 0)
    for d, out in enumerate(outs):
        named, rank = ranks(routes_t, own ^ d)
        hit = (slots == rank.astype(jnp.int32)) & (jnp.broadcast_to(named, (CAP, count)) > 0.5)
        picked = jnp.where(hit, 1.0, 0.0).astype(BF16)
        out[...] = jnp.dot(picked, tokens_ref[...], preferred_element_type=F32).astype(BF16)


def pack(place, routes_t, tokens, parts):
    count, width = tokens.shape
    part = width // parts
    tokens = pltpu.with_memory_space_constraint(tokens, pltpu.HBM)
    return pl.pallas_call(
        pack_kernel,
        grid_spec=pltpu.PrefetchScalarGridSpec(
            num_scalar_prefetch=1,
            grid=(1,),
            in_specs=[
                pl.BlockSpec(routes_t.shape, lambda i, place: (0, 0)),
                pl.BlockSpec((count, part), lambda i, place: (0, place[1])),
            ],
            out_specs=[pl.BlockSpec((CAP, part), lambda i, place: (0, 0))] * EXPERTS,
        ),
        out_shape=[jax.ShapeDtypeStruct((CAP, part), BF16)] * EXPERTS,
        compiler_params=pltpu.CompilerParams(vmem_limit_bytes=4 * MIB),
        name="pack",
    )(place, routes_t, tokens)


def dequant_kernel(step, code, scale_hbm, out, sems, scale_sem, scale_ref, spread, split, column):
    rows, _ = out.shape
    blocks = scale_ref.shape[0]
    scale_copy = pltpu.make_async_copy(scale_hbm, scale_ref, scale_sem)
    scale_copy.start()
    copies = []
    for i in range(rows // step):
        at = pl.ds(i * step, step)
        copies.append(pltpu.make_async_copy(code.at[at], out.at[at], sems.at[i]))
    for copy in copies:
        copy.start()
    row = lax.broadcasted_iota(jnp.int32, spread.shape, 0)
    col = lax.broadcasted_iota(jnp.int32, spread.shape, 1)
    spread[...] = jnp.where(lax.rem(row, blocks) == lax.div(col, QB), 1.0, 0.0).astype(BF16)
    scale_copy.wait()
    scale = scale_ref[...]
    high = scale.astype(BF16).astype(F32)
    column[...] = scale.T
    split[...] = jnp.concatenate([high, scale - high], axis=0).T.astype(BF16)
    for i, copy in enumerate(copies):
        copy.wait()
        at = slice(i * step, (i + 1) * step)
        for n in range(blocks // 2):
            if n % 4 == 0:
                for b in (2 * n, 2 * n + 1):
                    cols = slice(b * QB, (b + 1) * QB)
                    out[at, cols] = (out[at, cols].astype(F32) * column[at, b : b + 1]).astype(BF16)
            else:
                cols = slice(2 * n * QB, 2 * (n + 1) * QB)
                wide = jnp.dot(split[at, :], spread[:, cols], preferred_element_type=F32)
                out[at, cols] = (out[at, cols].astype(F32) * wide).astype(BF16)


def dequant(code, scale_t):
    rows, width = code.shape
    blocks = scale_t.shape[0]
    step = min(512, rows)
    code = pltpu.with_memory_space_constraint(code, pltpu.HBM)
    scale_t = pltpu.with_memory_space_constraint(scale_t, pltpu.HBM)
    in_hbm = pl.BlockSpec(memory_space=pltpu.HBM)
    return pl.pallas_call(
        functools.partial(dequant_kernel, step),
        in_specs=[in_hbm, in_hbm],
        out_specs=whole(),
        out_shape=VMEM((rows, width), BF16),
        scratch_shapes=[
            pltpu.SemaphoreType.DMA((rows // step,)),
            pltpu.SemaphoreType.DMA,
            VMEM(scale_t.shape, F32),
            VMEM((2 * blocks, width), BF16),
            VMEM((rows, 2 * blocks), BF16),
            VMEM((rows, blocks), F32),
        ],
        compiler_params=pltpu.CompilerParams(vmem_limit_bytes=4 * MIB),
        cost_estimate=pl.CostEstimate(flops=5 * 10**9, bytes_accessed=2 * rows * width, transcendentals=0),
    )(code, scale_t)


def hidden_kernel(parts, groups, span, place, *refs):
    xs, (w_gate, w_up, out, staged) = refs[: groups * parts], refs[groups * parts :]
    part = xs[0].shape[1]
    low, high = span
    block = min(256, high - low)
    at = [pl.ds(pl.multiple_of(lax.rem(place[1] + p, parts) * part, part), part) for p in range(parts)]
    row = 0
    for g in range(groups):
        for p in range(parts):
            x = xs[g * parts + p]
            staged[row : row + x.shape[0], p * part : (p + 1) * part] = x[...]
        row += x.shape[0]
    for n in range((high - low) // block):
        cols = slice(low + n * block, low + (n + 1) * block)
        gate = up = None
        for p in range(parts):
            x = staged[:, p * part : (p + 1) * part]
            g = jnp.dot(x, w_gate[at[p], cols], preferred_element_type=F32)
            u = jnp.dot(x, w_up[at[p], cols], preferred_element_type=F32)
            gate = g if gate is None else gate + g
            up = u if up is None else up + u
        out[:, n * block : (n + 1) * block] = (gate / (1.0 + jnp.exp(-gate)) * up).astype(BF16)


def hidden_of(place, xs, w_gate, w_up, span):
    parts = len(xs[0])
    flat = [x for group in xs for x in group]
    rows = sum(group[0].shape[0] for group in xs)
    width = span[1] - span[0]
    return pl.pallas_call(
        functools.partial(hidden_kernel, parts, len(xs), span),
        in_specs=[scalar()] + [whole()] * (len(flat) + 2),
        out_specs=whole(),
        out_shape=jax.ShapeDtypeStruct((rows, width), BF16),
        scratch_shapes=[VMEM((rows, w_gate.shape[0]), BF16)],
        compiler_params=pltpu.CompilerParams(vmem_limit_bytes=4 * MIB),
        cost_estimate=pl.CostEstimate(
            flops=4 * rows * w_gate.shape[0] * width, bytes_accessed=0, transcendentals=rows * width
        ),
    )(place, *flat, w_gate, w_up)


def down_kernel(count, shift, parts, place, *refs):
    hs, w, outs = refs[:count], refs[count], refs[count + 1 :]
    part = outs[0].shape[1]
    block = min(256, part)
    base = lax.rem(place[1] + shift, parts) * part
    for n in range(part // block):
        at = pl.ds(pl.multiple_of(base + n * block, block), block)
        total, low = None, 0
        for h in hs:
            got = jnp.dot(h[...], w[low : low + h.shape[1], at], preferred_element_type=F32)
            total = got if total is None else total + got
            low += h.shape[1]
        row = 0
        for out in outs:
            size = out.shape[0]
            out[:, n * block : (n + 1) * block] = total[row : row + size, :].astype(out.dtype)
            row += size


def down(place, hs, w, sizes, shift, parts, dtype):
    part = w.shape[1] // parts
    rows = sum(sizes)
    return pl.pallas_call(
        functools.partial(down_kernel, len(hs), shift, parts),
        in_specs=[scalar()] + [whole()] * (len(hs) + 1),
        out_specs=[whole()] * len(sizes),
        out_shape=[jax.ShapeDtypeStruct((size, part), dtype) for size in sizes],
        compiler_params=pltpu.CompilerParams(vmem_limit_bytes=4 * MIB),
        cost_estimate=pl.CostEstimate(flops=2 * rows * w.shape[0] * part, bytes_accessed=0, transcendentals=0),
    )(place, *hs, w)


def join_kernel(*refs):
    *ins, out = refs
    row = 0
    for ref in ins:
        out[row : row + ref.shape[0], :] = ref[...]
        row += ref.shape[0]


def join(xs):
    rows = sum(x.shape[0] for x in xs)
    return pl.pallas_call(
        join_kernel,
        in_specs=[whole()] * len(xs),
        out_specs=whole(),
        out_shape=jax.ShapeDtypeStruct((rows, xs[0].shape[1]), BF16),
        compiler_params=pltpu.CompilerParams(vmem_limit_bytes=2 * MIB),
    )(*xs)


def add_kernel(starts, *refs):
    *ins, out = refs
    rows = out.shape[0]
    total = None
    for start, ref in zip(starts, ins):
        term = ref[start : start + rows, :].astype(F32)
        total = term if total is None else total + term
    out[...] = total.astype(out.dtype)


def add_rows(terms, starts):
    return pl.pallas_call(
        functools.partial(add_kernel, starts),
        in_specs=[whole()] * len(terms),
        out_specs=whole(),
        out_shape=jax.ShapeDtypeStruct((CAP, terms[0].shape[1]), BF16),
        compiler_params=pltpu.CompilerParams(vmem_limit_bytes=1 * MIB),
    )(*terms)


def plan_kernel(place, routes_ref, weight_ref, *refs):
    *picks, weights = refs
    own = place[0]
    routes_t = routes_ref[...]
    count = routes_t.shape[1]
    weights[...] = weight_ref[...].T
    slots = lax.broadcasted_iota(jnp.int32, (CAP, TOP * count), 0)
    both = jnp.concatenate([routes_t[k : k + 1, :] for k in range(TOP)], axis=1)
    for d, pick in enumerate(picks):
        expert = own ^ d
        _, rank = ranks(routes_t, expert)
        wide = jnp.concatenate([rank] * TOP, axis=1).astype(jnp.int32)
        hit = (slots == wide) & (jnp.broadcast_to(both, slots.shape) == expert)
        pick[...] = jnp.where(hit, 1.0, 0.0).T.astype(BF16)


def plan(place, routes_t, weight_t):
    count = routes_t.shape[1]
    *picks, weights = pl.pallas_call(
        plan_kernel,
        in_specs=[scalar()] + [whole()] * 2,
        out_specs=[whole()] * (EXPERTS + 1),
        out_shape=[jax.ShapeDtypeStruct((TOP * count, CAP), BF16)] * EXPERTS
        + [jax.ShapeDtypeStruct((count, TOP), F32)],
        compiler_params=pltpu.CompilerParams(vmem_limit_bytes=4 * MIB),
        name="plan",
    )(place, routes_t, weight_t)
    return picks, weights


def mix_kernel(*refs):
    weights, *refs, out = refs
    picks, pieces = refs[:EXPERTS], refs[EXPERTS:]
    count = out.shape[0]
    gathered = None
    for pick, piece in zip(picks, pieces):
        got = jnp.dot(pick[...], piece[...], preferred_element_type=F32)
        gathered = got if gathered is None else gathered + got
    total = None
    for k in range(TOP):
        term = gathered[k * count : (k + 1) * count, :] * weights[:, k : k + 1]
        total = term if total is None else total + term
    out[...] = total.astype(BF16)


def mix(weights, picks, pieces):
    return pl.pallas_call(
        mix_kernel,
        in_specs=[whole()] * (1 + len(picks) + len(pieces)),
        out_specs=whole(),
        out_shape=jax.ShapeDtypeStruct((weights.shape[0], pieces[0].shape[1]), BF16),
        compiler_params=pltpu.CompilerParams(vmem_limit_bytes=4 * MIB),
        name="mix",
    )(weights, *picks, *pieces)


FAR, NEAR = (3, 2), (1, 0)


def layer(
    members, parts, tokens, routes, route_weight,
    gate_code, gate_scale, up_code, up_scale, down_code, down_scale,
):
    def send(x, where):
        pairs = []
        for e in range(EXPERTS):
            for m in range(members):
                for t in range(parts):
                    e2, m2, t2 = where(e, m, t)
                    pairs.append(((e * members + m) * parts + t, (e2 * members + m2) * parts + t2))
        return lax.ppermute(x, ("ep", "tp"), pairs)

    def to_expert(x, d):
        return x if d == 0 else send(x, lambda e, m, t: (e ^ d, m, t))

    def to_member(x, s):
        return x if s == 0 else send(x, lambda e, m, t: (e, (m + s) % members, t))

    def to_part(x, p):
        return x if p == 0 else send(x, lambda e, m, t: (e, m, (t + p) % parts))

    place = jnp.stack([lax.axis_index("ep") // members, lax.axis_index("tp")]).astype(jnp.int32)
    routes_t, weight_t = routes.T, route_weight.T
    order = FAR + NEAR
    groups = range(members)

    outgoing = pack(place, routes_t, tokens, parts)
    arrived = {d: to_expert(outgoing[d], d) for d in order}
    shared = {(s, d): to_member(arrived[d], s) for d in order for s in groups}

    w_gate = dequant(gate_code, gate_scale.T)
    w_up = dequant(up_code, up_scale.T)
    w_down = dequant(down_code, down_scale.T)

    def rows_of(chunk):
        xs = []
        for s in groups:
            own = join([shared[s, d] for d in chunk])
            xs.append([to_part(own, (parts - p) % parts) for p in range(parts)])
        return xs

    def reduced(chunk, hs):
        sizes = [CAP * len(chunk)] * members
        terms = [[] for _ in groups]
        for p in range(1, parts):
            partial = down(place, hs, w_down, sizes, p, parts, BF16)
            for s in reversed(groups):
                terms[s].append(to_part(partial[s], p))
        own = down(place, hs, w_down, sizes, 0, parts, F32)
        for s in groups:
            terms[s].append(own[s])
        return terms

    def returned(chunk, terms):
        pieces = {}
        for i, d in enumerate(chunk):
            start = i * CAP
            all_terms, starts = list(terms[0]), [start] * len(terms[0])
            for s in range(1, members):
                total = add_rows(terms[s], [start] * len(terms[s]))
                all_terms.append(to_member(total, members - s))
                starts.append(0)
            total = add_rows(all_terms, starts)
            pieces[d] = to_expert(total, d)
        return pieces

    units = w_gate.shape[1]
    far_hidden = hidden_of(place, rows_of(FAR), w_gate, w_up, (0, units))
    far_terms = reduced(FAR, [far_hidden])
    near_rows = rows_of(NEAR)
    half = units // 2
    near_hidden = [
        hidden_of(place, near_rows, w_gate, w_up, (0, half)),
        hidden_of(place, near_rows, w_gate, w_up, (half, units)),
    ]
    pieces = returned(FAR, far_terms)
    near_terms = reduced(NEAR, near_hidden)
    pieces.update(returned(NEAR, near_terms))
    picks, weights = plan(place, routes_t, weight_t)
    return mix(weights, picks, [pieces[d] for d in range(EXPERTS)])


def solution(mesh):
    members = mesh.shape["ep"] // EXPERTS
    parts = mesh.shape["tp"]
    rows = P(("rep", "ep"), None)
    columns = P(None, ("ep", "tp"))
    placed = (rows, rows, rows, columns, columns, columns, columns, P(("ep", "tp"), None), P(("ep", "tp"), None))

    def body(*args):
        return layer(members, parts, *args)

    return jax.shard_map(
        body, mesh=mesh, in_specs=placed, out_specs=P(("rep", "ep"), "tp"), check_vma=False
    )
```

```python
import functools

import jax
import jax.numpy as jnp
from jax import lax
from jax.experimental import pallas as pl
from jax.experimental.pallas import tpu as pltpu
from jax.sharding import PartitionSpec as P

EXPERTS = 4
TOP = 2
QB = 128
CAP = 40
F32 = jnp.float32
BF16 = jnp.bfloat16
VMEM = pltpu.VMEM
MIB = 2**20
LANES = 128


def whole():
    return pl.BlockSpec(memory_space=VMEM)


def scalar():
    return pl.BlockSpec(memory_space=pltpu.SMEM)


def ranks(routes_t, expert):
    count = routes_t.shape[1]
    named = (routes_t[0:1, :] == expert).astype(F32)
    for k in range(1, TOP):
        named = named + (routes_t[k : k + 1, :] == expert).astype(F32)
    rows = lax.broadcasted_iota(jnp.int32, (count, count), 0)
    cols = lax.broadcasted_iota(jnp.int32, (count, count), 1)
    earlier = (rows < cols).astype(F32)
    wide = jnp.broadcast_to(named, (8, count))
    return named, jnp.dot(wide, earlier, preferred_element_type=F32)[0:1, :]


def pack_kernel(place, routes_ref, tokens_ref, *outs):
    own = place[0]
    routes_t = routes_ref[...]
    count = routes_t.shape[1]
    slots = lax.broadcasted_iota(jnp.int32, (CAP, count), 0)
    for d, out in enumerate(outs):
        named, rank = ranks(routes_t, own ^ d)
        hit = (slots == rank.astype(jnp.int32)) & (jnp.broadcast_to(named, (CAP, count)) > 0.5)
        picked = jnp.where(hit, 1.0, 0.0).astype(BF16)
        out[...] = jnp.dot(picked, tokens_ref[...], preferred_element_type=F32).astype(BF16)


def pack(place, routes_t, tokens, parts):
    count, width = tokens.shape
    part = width // parts
    tokens = pltpu.with_memory_space_constraint(tokens, pltpu.HBM)
    return pl.pallas_call(
        pack_kernel,
        grid_spec=pltpu.PrefetchScalarGridSpec(
            num_scalar_prefetch=1,
            grid=(1,),
            in_specs=[
                pl.BlockSpec(routes_t.shape, lambda i, place: (0, 0)),
                pl.BlockSpec((count, part), lambda i, place: (0, place[1])),
            ],
            out_specs=[pl.BlockSpec((CAP, part), lambda i, place: (0, 0))] * EXPERTS,
        ),
        out_shape=[jax.ShapeDtypeStruct((CAP, part), BF16)] * EXPERTS,
        compiler_params=pltpu.CompilerParams(vmem_limit_bytes=1 * MIB),
        cost_estimate=pl.CostEstimate(flops=6 * 10**9, bytes_accessed=0, transcendentals=0),
        name="pack",
    )(place, routes_t, tokens)


def dequant_kernel(step, ahead, code, scale_ref, out, spread, split, column, sems=None):
    rows, _ = out.shape
    blocks = scale_ref.shape[0]
    pieces = [pl.ds(i * step, step) for i in range(rows // step)]
    copies = []
    if ahead:
        copies = [pltpu.make_async_copy(code.at[at], out.at[at], sems.at[i]) for i, at in enumerate(pieces)]
        code = out
    for copy in copies[:ahead]:
        copy.start()
    row = lax.broadcasted_iota(jnp.int32, spread.shape, 0)
    col = lax.broadcasted_iota(jnp.int32, spread.shape, 1)
    spread[...] = jnp.where(lax.rem(row, blocks) == lax.div(col, QB), 1.0, 0.0).astype(BF16)
    scale = scale_ref[...]
    high = scale.astype(BF16).astype(F32)
    column[...] = scale.T
    split[...] = jnp.concatenate([high, scale - high], axis=0).T.astype(BF16)
    for i in range(rows // step):
        if ahead:
            copies[i].wait()
            if i + ahead < len(copies):
                copies[i + ahead].start()
        at = slice(i * step, (i + 1) * step)
        for n in range(blocks // 2):
            if n % 4 == 0:
                for b in (2 * n, 2 * n + 1):
                    cols = slice(b * QB, (b + 1) * QB)
                    out[at, cols] = (code[at, cols].astype(F32) * column[at, b : b + 1]).astype(BF16)
            else:
                cols = slice(2 * n * QB, 2 * (n + 1) * QB)
                wide = jnp.dot(split[at, :], spread[:, cols], preferred_element_type=F32)
                out[at, cols] = (code[at, cols].astype(F32) * wide).astype(BF16)


def dequant(code, scale_t, ahead):
    rows, width = code.shape
    blocks = scale_t.shape[0]
    step = min(512, rows)
    first, sems = whole(), []
    if ahead:
        code = pltpu.with_memory_space_constraint(code, pltpu.HBM)
        first = pl.BlockSpec(memory_space=pltpu.HBM)
        sems = [pltpu.SemaphoreType.DMA((rows // step,))]
    return pl.pallas_call(
        functools.partial(dequant_kernel, step, ahead),
        in_specs=[first, whole()],
        out_specs=whole(),
        out_shape=VMEM((rows, width), BF16),
        scratch_shapes=[
            VMEM((2 * blocks, width), BF16),
            VMEM((rows, 2 * blocks), BF16),
            VMEM((rows, blocks), F32),
            *sems,
        ],
        compiler_params=pltpu.CompilerParams(vmem_limit_bytes=MIB // 2 + 6 * LANES * rows),
        cost_estimate=pl.CostEstimate(flops=5 * 10**9, bytes_accessed=2 * rows * width, transcendentals=0),
    )(code, scale_t)


def hidden_kernel(parts, groups, span, place, *refs):
    xs, (w_gate, w_up, out, staged) = refs[: groups * parts], refs[groups * parts :]
    part = xs[0].shape[1]
    low, high = span
    block = min(256, high - low)
    at = [pl.ds(pl.multiple_of(lax.rem(place[1] + p, parts) * part, part), part) for p in range(parts)]
    row = 0
    for g in range(groups):
        for p in range(parts):
            x = xs[g * parts + p]
            staged[row : row + x.shape[0], p * part : (p + 1) * part] = x[...]
        row += x.shape[0]
    for n in range((high - low) // block):
        cols = slice(low + n * block, low + (n + 1) * block)
        gate = up = None
        for p in range(parts):
            x = staged[:, p * part : (p + 1) * part]
            g = jnp.dot(x, w_gate[at[p], cols], preferred_element_type=F32)
            u = jnp.dot(x, w_up[at[p], cols], preferred_element_type=F32)
            gate = g if gate is None else gate + g
            up = u if up is None else up + u
        out[:, n * block : (n + 1) * block] = (gate / (1.0 + jnp.exp(-gate)) * up).astype(BF16)


def hidden_of(place, xs, w_gate, w_up, span):
    parts = len(xs[0])
    flat = [x for group in xs for x in group]
    rows = sum(group[0].shape[0] for group in xs)
    depth, width = w_gate.shape[0], span[1] - span[0]
    return pl.pallas_call(
        functools.partial(hidden_kernel, parts, len(xs), span),
        in_specs=[scalar()] + [whole()] * (len(flat) + 2),
        out_specs=whole(),
        out_shape=jax.ShapeDtypeStruct((rows, width), BF16),
        scratch_shapes=[VMEM((rows, w_gate.shape[0]), BF16)],
        compiler_params=pltpu.CompilerParams(vmem_limit_bytes=2 * MIB + 2 * rows * depth + MIB // 8),
        cost_estimate=pl.CostEstimate(
            flops=4 * rows * w_gate.shape[0] * width, bytes_accessed=0, transcendentals=rows * width
        ),
    )(place, *flat, w_gate, w_up)


def down_kernel(count, shift, parts, place, *refs):
    hs, w, outs = refs[:count], refs[count], refs[count + 1 :]
    part = outs[0].shape[1]
    block = min(256, part)
    base = lax.rem(place[1] + shift, parts) * part
    for n in range(part // block):
        at = pl.ds(pl.multiple_of(base + n * block, block), block)
        total, low = None, 0
        for h in hs:
            got = jnp.dot(h[...], w[low : low + h.shape[1], at], preferred_element_type=F32)
            total = got if total is None else total + got
            low += h.shape[1]
        row = 0
        for out in outs:
            size = out.shape[0]
            out[:, n * block : (n + 1) * block] = total[row : row + size, :].astype(out.dtype)
            row += size


def down(place, hs, w, sizes, shift, parts, dtype):
    part = w.shape[1] // parts
    rows = sum(sizes)
    return pl.pallas_call(
        functools.partial(down_kernel, len(hs), shift, parts),
        in_specs=[scalar()] + [whole()] * (len(hs) + 1),
        out_specs=[whole()] * len(sizes),
        out_shape=[jax.ShapeDtypeStruct((size, part), dtype) for size in sizes],
        compiler_params=pltpu.CompilerParams(vmem_limit_bytes=1 * MIB),
        cost_estimate=pl.CostEstimate(flops=2 * rows * w.shape[0] * part, bytes_accessed=0, transcendentals=0),
    )(place, *hs, w)


def join_kernel(*refs):
    *ins, out = refs
    row = 0
    for ref in ins:
        out[row : row + ref.shape[0], :] = ref[...]
        row += ref.shape[0]


def join(xs):
    rows = sum(x.shape[0] for x in xs)
    return pl.pallas_call(
        join_kernel,
        in_specs=[whole()] * len(xs),
        out_specs=whole(),
        out_shape=jax.ShapeDtypeStruct((rows, xs[0].shape[1]), BF16),
        compiler_params=pltpu.CompilerParams(vmem_limit_bytes=1 * MIB),
    )(*xs)


def add_kernel(count, starts, *refs):
    ins, outs = refs[:count], refs[count:]
    for start, out in zip(starts, outs):
        total = None
        for at, ref in zip(start, ins):
            term = ref[at : at + CAP, :].astype(F32)
            total = term if total is None else total + term
        out[...] = total.astype(out.dtype)


def add_rows(terms, starts):
    return pl.pallas_call(
        functools.partial(add_kernel, len(terms), starts),
        in_specs=[whole()] * len(terms),
        out_specs=[whole()] * len(starts),
        out_shape=[jax.ShapeDtypeStruct((CAP, terms[0].shape[1]), BF16)] * len(starts),
        compiler_params=pltpu.CompilerParams(vmem_limit_bytes=1 * MIB),
    )(*terms)


def plan_kernel(place, routes_ref, weight_ref, *refs):
    *picks, weights = refs
    own = place[0]
    routes_t = routes_ref[...]
    count = routes_t.shape[1]
    weights[...] = weight_ref[...].T
    slots = lax.broadcasted_iota(jnp.int32, (CAP, TOP * count), 0)
    both = jnp.concatenate([routes_t[k : k + 1, :] for k in range(TOP)], axis=1)
    for d, pick in enumerate(picks):
        expert = own ^ d
        _, rank = ranks(routes_t, expert)
        wide = jnp.concatenate([rank] * TOP, axis=1).astype(jnp.int32)
        hit = (slots == wide) & (jnp.broadcast_to(both, slots.shape) == expert)
        pick[...] = jnp.where(hit, 1.0, 0.0).T.astype(BF16)


def plan(place, routes_t, weight_t):
    count = routes_t.shape[1]
    *picks, weights = pl.pallas_call(
        plan_kernel,
        in_specs=[scalar()] + [whole()] * 2,
        out_specs=[whole()] * (EXPERTS + 1),
        out_shape=[jax.ShapeDtypeStruct((TOP * count, CAP), BF16)] * EXPERTS
        + [jax.ShapeDtypeStruct((count, TOP), F32)],
        compiler_params=pltpu.CompilerParams(vmem_limit_bytes=4 * MIB),
        name="plan",
    )(place, routes_t, weight_t)
    return picks, weights


def mix_kernel(owners, *refs):
    weights, *refs, out = refs
    picks, pieces = refs[:EXPERTS], refs[EXPERTS:]
    count = out.shape[0]
    gathered = None
    for d, piece in zip(owners, pieces):
        got = jnp.dot(picks[d][...], piece[...], preferred_element_type=F32)
        gathered = got if gathered is None else gathered + got
    total = None
    for k in range(TOP):
        term = gathered[k * count : (k + 1) * count, :] * weights[:, k : k + 1]
        total = term if total is None else total + term
    out[...] = total.astype(BF16)


def mix(weights, picks, pieces):
    owners = [d for d in range(EXPERTS) for _ in pieces[d]]
    pieces = [x for d in range(EXPERTS) for x in pieces[d]]
    return pl.pallas_call(
        functools.partial(mix_kernel, owners),
        in_specs=[whole()] * (1 + len(picks) + len(pieces)),
        out_specs=whole(),
        out_shape=jax.ShapeDtypeStruct((weights.shape[0], pieces[0].shape[1]), BF16),
        compiler_params=pltpu.CompilerParams(vmem_limit_bytes=2 * MIB),
        name="mix",
    )(weights, *picks, *pieces)


FAR, NEAR = (3, 2), (1, 0)


def layer(
    members, parts, tokens, routes, route_weight,
    gate_code, gate_scale, up_code, up_scale, down_code, down_scale,
):
    def send(x, where):
        pairs = []
        for e in range(EXPERTS):
            for m in range(members):
                for t in range(parts):
                    e2, m2, t2 = where(e, m, t)
                    pairs.append(((e * members + m) * parts + t, (e2 * members + m2) * parts + t2))
        return lax.ppermute(x, ("ep", "tp"), pairs)

    def to_expert(x, d):
        return x if d == 0 else send(x, lambda e, m, t: (e ^ d, m, t))

    def to_member(x, s):
        return x if s == 0 else send(x, lambda e, m, t: (e, (m + s) % members, t))

    def to_part(x, p):
        return x if p == 0 else send(x, lambda e, m, t: (e, m, (t + p) % parts))

    place = jnp.stack([lax.axis_index("ep") // members, lax.axis_index("tp")]).astype(jnp.int32)
    routes_t, weight_t = routes.T, route_weight.T
    order = FAR + NEAR
    groups = range(members)

    outgoing = pack(place, routes_t, tokens, parts)
    arrived = {d: to_expert(outgoing[d], d) for d in order}

    w_gate = dequant(gate_code, gate_scale.T, 0)
    w_up = dequant(up_code, up_scale.T, 0)
    w_down = dequant(down_code, down_scale.T, 3)

    def rows_of(chunk):
        joined = join([arrived[d] for d in chunk])
        xs = []
        for s in groups:
            own = to_member(joined, s)
            xs.append([to_part(own, (parts - p) % parts) for p in range(parts)])
        return xs

    def reduced(hs, sizes):
        terms = [[] for _ in sizes]
        for p in range(1, parts):
            partial = down(place, hs, w_down, sizes, p, parts, BF16)
            for k in reversed(range(len(sizes))):
                terms[k].append(to_part(partial[k], p))
        own = down(place, hs, w_down, sizes, 0, parts, F32)
        for k in range(len(sizes)):
            terms[k].append(own[k])
        return terms

    units = w_gate.shape[1]
    far_hidden = hidden_of(place, rows_of(FAR), w_gate, w_up, (0, units))
    far_terms = reduced([far_hidden], [CAP * len(FAR)] * members)
    near_rows = rows_of(NEAR)
    half = units // 2
    near_hidden = [
        hidden_of(place, near_rows, w_gate, w_up, (0, half)), hidden_of(place, near_rows, w_gate, w_up, (half, units))
    ]
    pieces = [[] for _ in range(EXPERTS)]
    for i, d in enumerate(FAR):
        start = i * CAP
        terms, starts = list(far_terms[0]), [start] * len(far_terms[0])
        for s in range(1, members):
            (total,) = add_rows(far_terms[s], [[start] * len(far_terms[s])])
            terms.append(to_member(total, members - s))
            starts.append(0)
        (total,) = add_rows(terms, [starts])
        pieces[d].append(to_expert(total, d))
    (near_terms,) = reduced(near_hidden, [CAP * len(NEAR) * members])
    slots = [(s, i) for s in groups for i in range(len(NEAR))]
    starts = [[(s * len(NEAR) + i) * CAP] * len(near_terms) for s, i in slots]
    for (s, i), total in zip(slots, add_rows(near_terms, starts)):
        d = NEAR[i]
        if s or d:
            total = send(total, lambda e, m, t, d=d, s=s: (e ^ d, (m + members - s) % members, t))
        pieces[d].append(total)
    picks, weights = plan(place, routes_t, weight_t)
    return mix(weights, picks, pieces)


def solution(mesh):
    members = mesh.shape["ep"] // EXPERTS
    parts = mesh.shape["tp"]
    rows = P(("rep", "ep"), None)
    columns = P(None, ("ep", "tp"))
    placed = (rows, rows, rows, columns, columns, columns, columns, P(("ep", "tp"), None), P(("ep", "tp"), None))

    def body(*args):
        return layer(members, parts, *args)

    return jax.shard_map(
        body, mesh=mesh, in_specs=placed, out_specs=P(("rep", "ep"), "tp"), check_vma=False
    )
```

```python
import functools
import math

import jax
import jax.numpy as jnp
from jax import lax
from jax.experimental import pallas as pl
from jax.experimental.pallas import tpu as pltpu
from jax.sharding import PartitionSpec as P

EXPERTS = 4
TOP = 2
QB = 128
CAP = 40
F32 = jnp.float32
BF16 = jnp.bfloat16
VMEM = pltpu.VMEM
MIB = 2**20
LANES = 128


def whole():
    return pl.BlockSpec(memory_space=VMEM)


def scalar():
    return pl.BlockSpec(memory_space=pltpu.SMEM)


def ranks(routes_t, expert):
    count = routes_t.shape[1]
    named = (routes_t[0:1, :] == expert).astype(F32)
    for k in range(1, TOP):
        named = named + (routes_t[k : k + 1, :] == expert).astype(F32)
    rows = lax.broadcasted_iota(jnp.int32, (count, count), 0)
    cols = lax.broadcasted_iota(jnp.int32, (count, count), 1)
    earlier = (rows < cols).astype(F32)
    wide = jnp.broadcast_to(named, (8, count))
    return named, jnp.dot(wide, earlier, preferred_element_type=F32)[0:1, :]


def pack_kernel(place, routes_hbm, tokens_hbm, *refs):
    *outs, routes_ref, tokens_ref, sems = refs
    own = place[0]
    count, part = tokens_ref.shape
    cols = pl.ds(pl.multiple_of(place[1] * part, part), part)
    routes_copy = pltpu.make_async_copy(routes_hbm, routes_ref, sems.at[0])
    tokens_copy = pltpu.make_async_copy(tokens_hbm.at[:, cols], tokens_ref, sems.at[1])
    routes_copy.start()
    tokens_copy.start()
    routes_copy.wait()
    routes_t = routes_ref[...]
    slots = lax.broadcasted_iota(jnp.int32, (CAP, count), 0)
    picks = []
    for d in range(len(outs)):
        named, rank = ranks(routes_t, own ^ d)
        hit = (slots == rank.astype(jnp.int32)) & (jnp.broadcast_to(named, (CAP, count)) > 0.5)
        picks.append(jnp.where(hit, 1.0, 0.0).astype(BF16))
    tokens_copy.wait()
    for picked, out in zip(picks, outs):
        out[...] = jnp.dot(picked, tokens_ref[...], preferred_element_type=F32).astype(BF16)


def pack(place, routes_t, tokens, parts):
    count, width = tokens.shape
    part = width // parts
    tokens = pltpu.with_memory_space_constraint(tokens, pltpu.HBM)
    routes_t = pltpu.with_memory_space_constraint(routes_t, pltpu.HBM)
    in_hbm = pl.BlockSpec(memory_space=pltpu.HBM)
    return pl.pallas_call(
        pack_kernel,
        in_specs=[scalar(), in_hbm, in_hbm],
        out_specs=[whole()] * EXPERTS,
        out_shape=[jax.ShapeDtypeStruct((CAP, part), BF16)] * EXPERTS,
        scratch_shapes=[VMEM(routes_t.shape, jnp.int32), VMEM((count, part), BF16), pltpu.SemaphoreType.DMA((2,))],
        compiler_params=pltpu.CompilerParams(vmem_limit_bytes=1 * MIB),
        cost_estimate=pl.CostEstimate(flops=6 * 10**9, bytes_accessed=0, transcendentals=0),
        name="pack",
    )(place, routes_t, tokens)


def dequant_kernel(step, early, ahead, code, scale_ref, *refs):
    refs = list(refs)
    other = refs.pop(0) if early or ahead is not None else None
    out = refs.pop(0)
    later = refs.pop(0) if early else None
    spread, split, column, sems = refs
    rows, _ = out.shape
    blocks = scale_ref.shape[0]

    def copy_of(piece, source, to):
        at = pl.ds(piece * step, step)
        return pltpu.make_async_copy(source.at[at], to.at[at], sems.at[piece])

    copies = [copy_of(i, other, later) for i in range(early)]
    if ahead is not None:
        copies = [copy_of(i, code, out) for i in range(ahead, rows // step)]
        code = out
    for copy in copies:
        copy.start()
    row = lax.broadcasted_iota(jnp.int32, spread.shape, 0)
    col = lax.broadcasted_iota(jnp.int32, spread.shape, 1)
    spread[...] = jnp.where(lax.rem(row, blocks) == lax.div(col, QB), 1.0, 0.0).astype(BF16)
    scale = scale_ref[...]
    high = scale.astype(BF16).astype(F32)
    column[...] = scale.T
    split[...] = jnp.concatenate([high, scale - high], axis=0).T.astype(BF16)
    for i in range(rows // step):
        if ahead is not None and i >= ahead:
            copies[i - ahead].wait()
        at = slice(i * step, (i + 1) * step)
        for n in range(blocks // 2):
            if n % 4 == 0:
                for b in (2 * n, 2 * n + 1):
                    cols = slice(b * QB, (b + 1) * QB)
                    out[at, cols] = (code[at, cols].astype(F32) * column[at, b : b + 1]).astype(BF16)
            else:
                cols = slice(2 * n * QB, 2 * (n + 1) * QB)
                wide = jnp.dot(split[at, :], spread[:, cols], preferred_element_type=F32)
                out[at, cols] = (code[at, cols].astype(F32) * wide).astype(BF16)
    if ahead is None:
        for copy in copies:
            copy.wait()


def dequant(code, scale_t, step, following=None, early=0, begun=None):
    rows, width = code.shape
    blocks = scale_t.shape[0]
    in_hbm = pl.BlockSpec(memory_space=pltpu.HBM)
    operands, specs = [code, scale_t], [whole(), whole()]
    outs, aliases = [VMEM((rows, width), BF16)], {}
    if early and following is not None:
        operands.append(pltpu.with_memory_space_constraint(following, pltpu.HBM))
        specs.append(in_hbm)
        outs.append(VMEM(following.shape, BF16))
        kernel = functools.partial(dequant_kernel, step, early, None)
    elif begun is not None:
        operands[0], specs[0] = pltpu.with_memory_space_constraint(code, pltpu.HBM), in_hbm
        operands.append(begun)
        specs.append(whole())
        aliases = {2: 0}
        kernel = functools.partial(dequant_kernel, step, 0, early)
    else:
        kernel = functools.partial(dequant_kernel, step, 0, None)
    return pl.pallas_call(
        kernel,
        in_specs=specs,
        out_specs=[whole()] * len(outs),
        out_shape=outs,
        input_output_aliases=aliases,
        scratch_shapes=[
            VMEM((2 * blocks, width), BF16),
            VMEM((rows, 2 * blocks), BF16),
            VMEM((rows, blocks), F32),
            pltpu.SemaphoreType.DMA((max(rows, 1 if following is None else following.shape[0]) // step,)),
        ],
        compiler_params=pltpu.CompilerParams(vmem_limit_bytes=MIB // 2 + 6 * LANES * rows),
        cost_estimate=pl.CostEstimate(flops=5 * 10**9, bytes_accessed=2 * rows * width, transcendentals=0),
    )(*operands)


def hidden_kernel(parts, groups, span, place, *refs):
    xs, (w_gate, w_up, out, staged) = refs[: groups * parts], refs[groups * parts :]
    part = xs[0].shape[1]
    low, high = span
    block = min(256, high - low)
    at = [pl.ds(pl.multiple_of(lax.rem(place[1] + p, parts) * part, part), part) for p in range(parts)]
    row = 0
    for g in range(groups):
        for p in range(parts):
            x = xs[g * parts + p]
            staged[row : row + x.shape[0], p * part : (p + 1) * part] = x[...]
        row += x.shape[0]
    for n in range((high - low) // block):
        cols = slice(low + n * block, low + (n + 1) * block)
        gate = up = None
        for p in range(parts):
            x = staged[:, p * part : (p + 1) * part]
            g = jnp.dot(x, w_gate[at[p], cols], preferred_element_type=F32)
            u = jnp.dot(x, w_up[at[p], cols], preferred_element_type=F32)
            gate = g if gate is None else gate + g
            up = u if up is None else up + u
        out[:, n * block : (n + 1) * block] = (gate / (1.0 + jnp.exp(-gate)) * up).astype(BF16)


def hidden_of(place, xs, w_gate, w_up, span):
    parts = len(xs[0])
    flat = [x for group in xs for x in group]
    rows = sum(group[0].shape[0] for group in xs)
    depth, width = w_gate.shape[0], span[1] - span[0]
    return pl.pallas_call(
        functools.partial(hidden_kernel, parts, len(xs), span),
        in_specs=[scalar()] + [whole()] * (len(flat) + 2),
        out_specs=whole(),
        out_shape=jax.ShapeDtypeStruct((rows, width), BF16),
        scratch_shapes=[VMEM((rows, w_gate.shape[0]), BF16)],
        compiler_params=pltpu.CompilerParams(vmem_limit_bytes=2 * MIB + 2 * rows * depth + MIB // 8),
        cost_estimate=pl.CostEstimate(
            flops=4 * rows * w_gate.shape[0] * width, bytes_accessed=0, transcendentals=rows * width
        ),
    )(place, *flat, w_gate, w_up)


def down_kernel(count, shift, parts, place, *refs):
    hs, w, outs = refs[:count], refs[count], refs[count + 1 :]
    part = outs[0].shape[1]
    block = min(256, part)
    base = lax.rem(place[1] + shift, parts) * part
    for n in range(part // block):
        at = pl.ds(pl.multiple_of(base + n * block, block), block)
        total, low = None, 0
        for h in hs:
            got = jnp.dot(h[...], w[low : low + h.shape[1], at], preferred_element_type=F32)
            total = got if total is None else total + got
            low += h.shape[1]
        row = 0
        for out in outs:
            size = out.shape[0]
            out[:, n * block : (n + 1) * block] = total[row : row + size, :].astype(out.dtype)
            row += size


def down(place, hs, w, sizes, shift, parts, dtype):
    part = w.shape[1] // parts
    rows = sum(sizes)
    return pl.pallas_call(
        functools.partial(down_kernel, len(hs), shift, parts),
        in_specs=[scalar()] + [whole()] * (len(hs) + 1),
        out_specs=[whole()] * len(sizes),
        out_shape=[jax.ShapeDtypeStruct((size, part), dtype) for size in sizes],
        compiler_params=pltpu.CompilerParams(vmem_limit_bytes=1 * MIB),
        cost_estimate=pl.CostEstimate(flops=2 * rows * w.shape[0] * part, bytes_accessed=0, transcendentals=0),
    )(place, *hs, w)


def join_kernel(*refs):
    *ins, out = refs
    row = 0
    for ref in ins:
        out[row : row + ref.shape[0], :] = ref[...]
        row += ref.shape[0]


def join(xs):
    rows = sum(x.shape[0] for x in xs)
    return pl.pallas_call(
        join_kernel,
        in_specs=[whole()] * len(xs),
        out_specs=whole(),
        out_shape=jax.ShapeDtypeStruct((rows, xs[0].shape[1]), BF16),
        compiler_params=pltpu.CompilerParams(vmem_limit_bytes=1 * MIB),
    )(*xs)


def add_kernel(count, starts, *refs):
    ins, outs = refs[:count], refs[count:]
    for start, out in zip(starts, outs):
        total = None
        for at, ref in zip(start, ins):
            term = ref[at : at + CAP, :].astype(F32)
            total = term if total is None else total + term
        out[...] = total.astype(out.dtype)


def add_rows(terms, starts):
    return pl.pallas_call(
        functools.partial(add_kernel, len(terms), starts),
        in_specs=[whole()] * len(terms),
        out_specs=[whole()] * len(starts),
        out_shape=[jax.ShapeDtypeStruct((CAP, terms[0].shape[1]), BF16)] * len(starts),
        compiler_params=pltpu.CompilerParams(vmem_limit_bytes=1 * MIB),
    )(*terms)


def plan_kernel(place, routes_ref, weight_ref, *refs):
    *picks, weights = refs
    own = place[0]
    routes_t = routes_ref[...]
    count = routes_t.shape[1]
    weights[...] = weight_ref[...].T
    slots = lax.broadcasted_iota(jnp.int32, (CAP, TOP * count), 0)
    both = jnp.concatenate([routes_t[k : k + 1, :] for k in range(TOP)], axis=1)
    for d, pick in enumerate(picks):
        expert = own ^ d
        _, rank = ranks(routes_t, expert)
        wide = jnp.concatenate([rank] * TOP, axis=1).astype(jnp.int32)
        hit = (slots == wide) & (jnp.broadcast_to(both, slots.shape) == expert)
        pick[...] = jnp.where(hit, 1.0, 0.0).T.astype(BF16)


def plan(place, routes_t, weight_t):
    count = routes_t.shape[1]
    *picks, weights = pl.pallas_call(
        plan_kernel,
        in_specs=[scalar()] + [whole()] * 2,
        out_specs=[whole()] * (EXPERTS + 1),
        out_shape=[jax.ShapeDtypeStruct((TOP * count, CAP), BF16)] * EXPERTS
        + [jax.ShapeDtypeStruct((count, TOP), F32)],
        compiler_params=pltpu.CompilerParams(vmem_limit_bytes=4 * MIB),
        name="plan",
    )(place, routes_t, weight_t)
    return picks, weights


def mix_kernel(owners, *refs):
    weights, *refs, out = refs
    picks, pieces = refs[:EXPERTS], refs[EXPERTS:]
    count = out.shape[0]
    gathered = None
    for d, piece in zip(owners, pieces):
        got = jnp.dot(picks[d][...], piece[...], preferred_element_type=F32)
        gathered = got if gathered is None else gathered + got
    total = None
    for k in range(TOP):
        term = gathered[k * count : (k + 1) * count, :] * weights[:, k : k + 1]
        total = term if total is None else total + term
    out[...] = total.astype(BF16)


def mix(weights, picks, pieces):
    owners = [d for d in range(EXPERTS) for _ in pieces[d]]
    pieces = [x for d in range(EXPERTS) for x in pieces[d]]
    return pl.pallas_call(
        functools.partial(mix_kernel, owners),
        in_specs=[whole()] * (1 + len(picks) + len(pieces)),
        out_specs=whole(),
        out_shape=jax.ShapeDtypeStruct((weights.shape[0], pieces[0].shape[1]), BF16),
        compiler_params=pltpu.CompilerParams(vmem_limit_bytes=2 * MIB),
        name="mix",
    )(weights, *picks, *pieces)


FAR, NEAR = (3, 2), (1, 0)


def layer(
    members, parts, tokens, routes, route_weight,
    gate_code, gate_scale, up_code, up_scale, down_code, down_scale,
):
    def send(x, where):
        pairs = []
        for e in range(EXPERTS):
            for m in range(members):
                for t in range(parts):
                    e2, m2, t2 = where(e, m, t)
                    pairs.append(((e * members + m) * parts + t, (e2 * members + m2) * parts + t2))
        return lax.ppermute(x, ("ep", "tp"), pairs)

    def to_expert(x, d):
        return x if d == 0 else send(x, lambda e, m, t: (e ^ d, m, t))

    def to_member(x, s):
        return x if s == 0 else send(x, lambda e, m, t: (e, (m + s) % members, t))

    def to_part(x, p):
        return x if p == 0 else send(x, lambda e, m, t: (e, m, (t + p) % parts))

    place = jnp.stack([lax.axis_index("ep") // members, lax.axis_index("tp")]).astype(jnp.int32)
    routes_t, weight_t = routes.T, route_weight.T
    order = FAR + NEAR
    groups = range(members)

    outgoing = pack(place, routes_t, tokens, parts)
    arrived = {d: to_expert(outgoing[d], d) for d in order}

    step = math.gcd(math.gcd(gate_code.shape[0], down_code.shape[0]), 512)
    early = max(1, down_code.shape[0] // step // 2)
    (w_gate,) = dequant(gate_code, gate_scale.T, step)
    w_up, begun = dequant(up_code, up_scale.T, step, following=down_code, early=early)
    (w_down,) = dequant(down_code, down_scale.T, step, early=early, begun=begun)

    def rows_of(chunks):
        xs = []
        for s in groups:
            for chunk in chunks if s else [sum(chunks, ())]:
                own = join([arrived[d] for d in chunk]) if len(chunk) > 1 else arrived[chunk[0]]
                own = to_member(own, s)
                xs.append([to_part(own, (parts - p) % parts) for p in range(parts)])
        return xs

    def reduced(hs, sizes):
        terms = [[] for _ in sizes]
        for p in range(1, parts):
            partial = down(place, hs, w_down, sizes, p, parts, BF16)
            for k in reversed(range(len(sizes))):
                terms[k].append(to_part(partial[k], p))
        own = down(place, hs, w_down, sizes, 0, parts, F32)
        for k in range(len(sizes)):
            terms[k].append(own[k])
        return terms

    units = w_gate.shape[1]
    far_hidden = hidden_of(place, rows_of([(d,) for d in FAR]), w_gate, w_up, (0, units))
    far_terms = reduced([far_hidden], [CAP * len(FAR)] * members)
    near_rows = rows_of([NEAR])
    near_hidden = hidden_of(place, near_rows, w_gate, w_up, (0, units))
    pieces = [[] for _ in range(EXPERTS)]
    for i, d in enumerate(FAR):
        start = i * CAP
        terms, starts = list(far_terms[0]), [start] * len(far_terms[0])
        for s in range(1, members):
            (total,) = add_rows(far_terms[s], [[start] * len(far_terms[s])])
            terms.append(to_member(total, members - s))
            starts.append(0)
        (total,) = add_rows(terms, [starts])
        pieces[d].append(to_expert(total, d))
    (near_terms,) = reduced([near_hidden], [CAP * len(NEAR) * members])
    slots = [(s, i) for s in groups for i in range(len(NEAR))]
    starts = [[(s * len(NEAR) + i) * CAP] * len(near_terms) for s, i in slots]
    for (s, i), total in zip(slots, add_rows(near_terms, starts)):
        d = NEAR[i]
        if s or d:
            total = send(total, lambda e, m, t, d=d, s=s: (e ^ d, (m + members - s) % members, t))
        pieces[d].append(total)
    picks, weights = plan(place, routes_t, weight_t)
    return mix(weights, picks, pieces)


def solution(mesh):
    members = mesh.shape["ep"] // EXPERTS
    parts = mesh.shape["tp"]
    rows = P(("rep", "ep"), None)
    columns = P(None, ("ep", "tp"))
    placed = (rows, rows, rows, columns, columns, columns, columns, P(("ep", "tp"), None), P(("ep", "tp"), None))

    def body(*args):
        return layer(members, parts, *args)

    return jax.shard_map(
        body, mesh=mesh, in_specs=placed, out_specs=P(("rep", "ep"), "tp"), check_vma=False
    )
```

```python
import functools
import math

import jax
import jax.numpy as jnp
from jax import lax
from jax.experimental import pallas as pl
from jax.experimental.pallas import tpu as pltpu
from jax.sharding import PartitionSpec as P

EXPERTS = 4
TOP = 2
QB = 128
CAP = 40
F32 = jnp.float32
BF16 = jnp.bfloat16
VMEM = pltpu.VMEM
MIB = 2**20
LANES = 128


def whole():
    return pl.BlockSpec(memory_space=VMEM)


def scalar():
    return pl.BlockSpec(memory_space=pltpu.SMEM)


def ranks(routes_t, expert):
    count = routes_t.shape[1]
    named = (routes_t[0:1, :] == expert).astype(F32)
    for k in range(1, TOP):
        named = named + (routes_t[k : k + 1, :] == expert).astype(F32)
    rows = lax.broadcasted_iota(jnp.int32, (count, count), 0)
    cols = lax.broadcasted_iota(jnp.int32, (count, count), 1)
    earlier = (rows < cols).astype(F32)
    wide = jnp.broadcast_to(named, (8, count))
    return named, jnp.dot(wide, earlier, preferred_element_type=F32)[0:1, :]


def pack_kernel(place, routes_hbm, tokens_hbm, *refs):
    *outs, routes_ref, tokens_ref, sems = refs
    own = place[0]
    count, part = tokens_ref.shape
    cols = pl.ds(pl.multiple_of(place[1] * part, part), part)
    routes_copy = pltpu.make_async_copy(routes_hbm, routes_ref, sems.at[0])
    tokens_copy = pltpu.make_async_copy(tokens_hbm.at[:, cols], tokens_ref, sems.at[1])
    routes_copy.start()
    tokens_copy.start()
    routes_copy.wait()
    routes_t = routes_ref[...]
    slots = lax.broadcasted_iota(jnp.int32, (CAP, count), 0)
    picks = []
    for d in range(len(outs)):
        named, rank = ranks(routes_t, own ^ d)
        hit = (slots == rank.astype(jnp.int32)) & (jnp.broadcast_to(named, (CAP, count)) > 0.5)
        picks.append(jnp.where(hit, 1.0, 0.0).astype(BF16))
    tokens_copy.wait()
    for picked, out in zip(picks, outs):
        out[...] = jnp.dot(picked, tokens_ref[...], preferred_element_type=F32).astype(BF16)


def pack(place, routes_t, tokens, parts):
    count, width = tokens.shape
    part = width // parts
    tokens = pltpu.with_memory_space_constraint(tokens, pltpu.HBM)
    routes_t = pltpu.with_memory_space_constraint(routes_t, pltpu.HBM)
    in_hbm = pl.BlockSpec(memory_space=pltpu.HBM)
    return pl.pallas_call(
        pack_kernel,
        in_specs=[scalar(), in_hbm, in_hbm],
        out_specs=[whole()] * EXPERTS,
        out_shape=[jax.ShapeDtypeStruct((CAP, part), BF16)] * EXPERTS,
        scratch_shapes=[VMEM(routes_t.shape, jnp.int32), VMEM((count, part), BF16), pltpu.SemaphoreType.DMA((2,))],
        compiler_params=pltpu.CompilerParams(vmem_limit_bytes=1 * MIB),
        cost_estimate=pl.CostEstimate(flops=6 * 10**9, bytes_accessed=0, transcendentals=0),
        name="pack",
    )(place, routes_t, tokens)


def dequant_kernel(step, early, ahead, code, scale_ref, *refs):
    refs = list(refs)
    other = refs.pop(0) if early or ahead is not None else None
    out = refs.pop(0)
    later = refs.pop(0) if early else None
    spread, split, column, sems = refs
    rows, _ = out.shape
    blocks = scale_ref.shape[0]

    def copy_of(piece, source, to):
        at = pl.ds(piece * step, step)
        return pltpu.make_async_copy(source.at[at], to.at[at], sems.at[piece])

    copies = [copy_of(i, other, later) for i in range(early)]
    if ahead is not None:
        copies = [copy_of(i, code, out) for i in range(ahead, rows // step)]
        code = out
    for copy in copies:
        copy.start()
    row = lax.broadcasted_iota(jnp.int32, spread.shape, 0)
    col = lax.broadcasted_iota(jnp.int32, spread.shape, 1)
    spread[...] = jnp.where(lax.rem(row, blocks) == lax.div(col, QB), 1.0, 0.0).astype(BF16)
    scale = scale_ref[...]
    high = scale.astype(BF16).astype(F32)
    column[...] = scale.T
    split[...] = jnp.concatenate([high, scale - high], axis=0).T.astype(BF16)
    for i in range(rows // step):
        if ahead is not None and i >= ahead:
            copies[i - ahead].wait()
        at = slice(i * step, (i + 1) * step)
        for n in range(blocks // 2):
            if n % 4 == 0:
                for b in (2 * n, 2 * n + 1):
                    cols = slice(b * QB, (b + 1) * QB)
                    out[at, cols] = (code[at, cols].astype(F32) * column[at, b : b + 1]).astype(BF16)
            else:
                cols = slice(2 * n * QB, 2 * (n + 1) * QB)
                wide = jnp.dot(split[at, :], spread[:, cols], preferred_element_type=F32)
                out[at, cols] = (code[at, cols].astype(F32) * wide).astype(BF16)
    if ahead is None:
        for copy in copies:
            copy.wait()


def dequant(code, scale_t, step, following=None, early=0, begun=None):
    rows, width = code.shape
    blocks = scale_t.shape[0]
    in_hbm = pl.BlockSpec(memory_space=pltpu.HBM)
    operands, specs = [code, scale_t], [whole(), whole()]
    outs, aliases = [VMEM((rows, width), BF16)], {}
    if early and following is not None:
        operands.append(pltpu.with_memory_space_constraint(following, pltpu.HBM))
        specs.append(in_hbm)
        outs.append(VMEM(following.shape, BF16))
        kernel = functools.partial(dequant_kernel, step, early, None)
    elif begun is not None:
        operands[0], specs[0] = pltpu.with_memory_space_constraint(code, pltpu.HBM), in_hbm
        operands.append(begun)
        specs.append(whole())
        aliases = {2: 0}
        kernel = functools.partial(dequant_kernel, step, 0, early)
    else:
        kernel = functools.partial(dequant_kernel, step, 0, None)
    return pl.pallas_call(
        kernel,
        in_specs=specs,
        out_specs=[whole()] * len(outs),
        out_shape=outs,
        input_output_aliases=aliases,
        scratch_shapes=[
            VMEM((2 * blocks, width), BF16),
            VMEM((rows, 2 * blocks), BF16),
            VMEM((rows, blocks), F32),
            pltpu.SemaphoreType.DMA((max(rows, 1 if following is None else following.shape[0]) // step,)),
        ],
        compiler_params=pltpu.CompilerParams(vmem_limit_bytes=MIB // 2 + 6 * LANES * rows),
        cost_estimate=pl.CostEstimate(flops=5 * 10**9, bytes_accessed=2 * rows * width, transcendentals=0),
    )(*operands)


def hidden_kernel(parts, groups, span, *refs):
    xs, (w_gate, w_up, out, staged) = refs[: groups * parts], refs[groups * parts :]
    part = xs[0].shape[1]
    low, high = span
    block = min(256, high - low)
    at = [pl.ds(pl.multiple_of(lax.rem(lax.axis_index("tp") + p, parts) * part, part), part) for p in range(parts)]
    row = 0
    for g in range(groups):
        for p in range(parts):
            x = xs[g * parts + p]
            staged[row : row + x.shape[0], p * part : (p + 1) * part] = x[...]
        row += x.shape[0]
    for n in range((high - low) // block):
        cols = slice(low + n * block, low + (n + 1) * block)
        gate = up = None
        for p in range(parts):
            x = staged[:, p * part : (p + 1) * part]
            g = jnp.dot(x, w_gate[at[p], cols], preferred_element_type=F32)
            u = jnp.dot(x, w_up[at[p], cols], preferred_element_type=F32)
            gate = g if gate is None else gate + g
            up = u if up is None else up + u
        out[:, n * block : (n + 1) * block] = (gate / (1.0 + jnp.exp(-gate)) * up).astype(BF16)


def hidden_of(xs, w_gate, w_up, span):
    parts = len(xs[0])
    flat = [x for group in xs for x in group]
    rows = sum(group[0].shape[0] for group in xs)
    depth, width = w_gate.shape[0], span[1] - span[0]
    return pl.pallas_call(
        functools.partial(hidden_kernel, parts, len(xs), span),
        in_specs=[whole()] * (len(flat) + 2),
        out_specs=whole(),
        out_shape=jax.ShapeDtypeStruct((rows, width), BF16),
        scratch_shapes=[VMEM((rows, w_gate.shape[0]), BF16)],
        compiler_params=pltpu.CompilerParams(vmem_limit_bytes=2 * MIB + 2 * rows * depth + MIB // 8),
        cost_estimate=pl.CostEstimate(
            flops=4 * rows * w_gate.shape[0] * width, bytes_accessed=0, transcendentals=rows * width
        ),
    )(*flat, w_gate, w_up)


def down_kernel(count, shift, parts, *refs):
    hs, w, outs = refs[:count], refs[count], refs[count + 1 :]
    part = outs[0].shape[1]
    block = math.gcd(part, 256)
    base = lax.rem(lax.axis_index("tp") + shift, parts) * part
    for n in range(part // block):
        at = pl.ds(pl.multiple_of(base + n * block, block), block)
        total, low = None, 0
        for h in hs:
            got = jnp.dot(h[...], w[low : low + h.shape[1], at], preferred_element_type=F32)
            total = got if total is None else total + got
            low += h.shape[1]
        row = 0
        for out in outs:
            size = out.shape[0]
            out[:, n * block : (n + 1) * block] = total[row : row + size, :].astype(out.dtype)
            row += size


def down(hs, w, sizes, shift, parts, dtype):
    part = w.shape[1] // parts
    rows = sum(sizes)
    return pl.pallas_call(
        functools.partial(down_kernel, len(hs), shift, parts),
        in_specs=[whole()] * (len(hs) + 1),
        out_specs=[whole()] * len(sizes),
        out_shape=[jax.ShapeDtypeStruct((size, part), dtype) for size in sizes],
        compiler_params=pltpu.CompilerParams(vmem_limit_bytes=1 * MIB),
        cost_estimate=pl.CostEstimate(flops=2 * rows * w.shape[0] * part, bytes_accessed=0, transcendentals=0),
    )(*hs, w)


def join_kernel(*refs):
    *ins, out = refs
    row = 0
    for ref in ins:
        out[row : row + ref.shape[0], :] = ref[...]
        row += ref.shape[0]


def join(xs):
    rows = sum(x.shape[0] for x in xs)
    return pl.pallas_call(
        join_kernel,
        in_specs=[whole()] * len(xs),
        out_specs=whole(),
        out_shape=jax.ShapeDtypeStruct((rows, xs[0].shape[1]), BF16),
        compiler_params=pltpu.CompilerParams(vmem_limit_bytes=1 * MIB),
    )(*xs)


def add_kernel(count, starts, *refs):
    ins, outs = refs[:count], refs[count:]
    for start, out in zip(starts, outs):
        total = None
        for at, ref in zip(start, ins):
            term = ref[at : at + CAP, :].astype(F32)
            total = term if total is None else total + term
        out[...] = total.astype(out.dtype)


def add_rows(terms, starts):
    return pl.pallas_call(
        functools.partial(add_kernel, len(terms), starts),
        in_specs=[whole()] * len(terms),
        out_specs=[whole()] * len(starts),
        out_shape=[jax.ShapeDtypeStruct((CAP, terms[0].shape[1]), BF16)] * len(starts),
        compiler_params=pltpu.CompilerParams(vmem_limit_bytes=1 * MIB),
    )(*terms)


def plan_kernel(members, routes_ref, weight_ref, *refs):
    *picks, weights = refs
    own = lax.axis_index("ep") // members
    routes_t = routes_ref[...]
    count = routes_t.shape[1]
    weights[...] = weight_ref[...].T
    slots = lax.broadcasted_iota(jnp.int32, (CAP, TOP * count), 0)
    both = jnp.concatenate([routes_t[k : k + 1, :] for k in range(TOP)], axis=1)
    for d, pick in enumerate(picks):
        expert = own ^ d
        _, rank = ranks(routes_t, expert)
        wide = jnp.concatenate([rank] * TOP, axis=1).astype(jnp.int32)
        hit = (slots == wide) & (jnp.broadcast_to(both, slots.shape) == expert)
        pick[...] = jnp.where(hit, 1.0, 0.0).T.astype(BF16)


def plan(members, routes_t, weight_t):
    count = routes_t.shape[1]
    *picks, weights = pl.pallas_call(
        functools.partial(plan_kernel, members),
        in_specs=[whole()] * 2,
        out_specs=[whole()] * (EXPERTS + 1),
        out_shape=[jax.ShapeDtypeStruct((TOP * count, CAP), BF16)] * EXPERTS
        + [jax.ShapeDtypeStruct((count, TOP), F32)],
        compiler_params=pltpu.CompilerParams(vmem_limit_bytes=4 * MIB),
        name="plan",
    )(routes_t, weight_t)
    return picks, weights


def gather_kernel(owners, *refs):
    picks, refs = refs[:EXPERTS], refs[EXPERTS:]
    pieces, refs = refs[: len(owners)], refs[len(owners) :]
    total = refs[0][...] if len(refs) == 2 else None
    for d, piece in zip(owners, pieces):
        got = jnp.dot(picks[d][...], piece[...], preferred_element_type=F32)
        total = got if total is None else total + got
    refs[-1][...] = total


def gather(picks, owners, pieces):
    return pl.pallas_call(
        functools.partial(gather_kernel, owners),
        in_specs=[whole()] * (len(picks) + len(pieces)),
        out_specs=whole(),
        out_shape=jax.ShapeDtypeStruct((picks[0].shape[0], pieces[0].shape[1]), F32),
        compiler_params=pltpu.CompilerParams(vmem_limit_bytes=2 * MIB),
    )(*picks, *pieces)


def mix_kernel(owners, early, weights, *refs):
    picks, refs = refs[:EXPERTS], refs[EXPERTS:]
    pieces, (out, staged, sems) = refs[: len(owners)], refs[len(owners) :]
    count, width = out.shape
    block = math.gcd(width, 512)
    copies = []
    for n in range(width // block):
        cols = slice(n * block, (n + 1) * block)
        gathered = early[:, cols]
        for d, piece in zip(owners, pieces):
            gathered = gathered + jnp.dot(picks[d][...], piece[:, cols], preferred_element_type=F32)
        total = None
        for k in range(TOP):
            term = gathered[k * count : (k + 1) * count, :] * weights[:, k : k + 1]
            total = term if total is None else total + term
        staged[:, cols] = total.astype(BF16)
        at = pl.ds(n * block, block)
        copies.append(pltpu.make_async_copy(staged.at[:, at], out.at[:, at], sems.at[n]))
        copies[-1].start()
    for copy in copies:
        copy.wait()


def mix(weights, picks, early, owners, pieces):
    count, width = weights.shape[0], early.shape[1]
    return pl.pallas_call(
        functools.partial(mix_kernel, owners),
        in_specs=[whole()] * (2 + len(picks) + len(pieces)),
        out_specs=pl.BlockSpec(memory_space=pltpu.HBM),
        out_shape=jax.ShapeDtypeStruct((count, width), BF16),
        scratch_shapes=[VMEM((count, width), BF16), pltpu.SemaphoreType.DMA((width // math.gcd(width, 512),))],
        compiler_params=pltpu.CompilerParams(vmem_limit_bytes=2 * MIB),
        name="mix",
    )(early, weights, *picks, *pieces)


FAR, NEAR = (3, 2), (1, 0)


def layer(
    members, parts, tokens, routes, route_weight,
    gate_code, gate_scale, up_code, up_scale, down_code, down_scale,
):
    def send(x, where):
        pairs = []
        for e in range(EXPERTS):
            for m in range(members):
                for t in range(parts):
                    e2, m2, t2 = where(e, m, t)
                    pairs.append(((e * members + m) * parts + t, (e2 * members + m2) * parts + t2))
        return lax.ppermute(x, ("ep", "tp"), pairs)

    def to_expert(x, d):
        return x if d == 0 else send(x, lambda e, m, t: (e ^ d, m, t))

    def to_member(x, s):
        return x if s == 0 else send(x, lambda e, m, t: (e, (m + s) % members, t))

    def to_part(x, p):
        return x if p == 0 else send(x, lambda e, m, t: (e, m, (t + p) % parts))

    place = jnp.stack([lax.axis_index("ep") // members, lax.axis_index("tp")]).astype(jnp.int32)
    routes_t, weight_t = routes.T, route_weight.T
    order = FAR + NEAR
    groups = range(members)

    outgoing = pack(place, routes_t, tokens, parts)
    arrived = {d: to_expert(outgoing[d], d) for d in order}

    step = math.gcd(math.gcd(gate_code.shape[0], down_code.shape[0]), 512)
    early = max(1, down_code.shape[0] // step // 2)
    (w_gate,) = dequant(gate_code, gate_scale.T, step)
    w_up, begun = dequant(up_code, up_scale.T, step, following=down_code, early=early)
    (w_down,) = dequant(down_code, down_scale.T, step, early=early, begun=begun)

    def rows_of(chunks):
        xs = []
        for s in groups:
            for chunk in chunks if s else [sum(chunks, ())]:
                own = join([arrived[d] for d in chunk]) if len(chunk) > 1 else arrived[chunk[0]]
                own = to_member(own, s)
                xs.append([to_part(own, (parts - p) % parts) for p in range(parts)])
        return xs

    def reduced(hs, sizes):
        terms = [[] for _ in sizes]
        for p in range(1, parts):
            partial = down(hs, w_down, sizes, p, parts, BF16)
            for k in reversed(range(len(sizes))):
                terms[k].append(to_part(partial[k], p))
        own = down(hs, w_down, sizes, 0, parts, F32)
        for k in range(len(sizes)):
            terms[k].append(own[k])
        return terms

    units = w_gate.shape[1]
    far_hidden = hidden_of(rows_of([(d,) for d in FAR]), w_gate, w_up, (0, units))
    far_terms = reduced([far_hidden], [CAP * len(FAR)] * members)
    near_rows = rows_of([NEAR])
    near_hidden = hidden_of(near_rows, w_gate, w_up, (0, units))
    pieces = [[] for _ in range(EXPERTS)]
    for i, d in enumerate(FAR):
        start = i * CAP
        terms, starts = list(far_terms[0]), [start] * len(far_terms[0])
        for s in range(1, members):
            (total,) = add_rows(far_terms[s], [[start] * len(far_terms[s])])
            terms.append(to_member(total, members - s))
            starts.append(0)
        (total,) = add_rows(terms, [starts])
        pieces[d].append(to_expert(total, d))
    (near_terms,) = reduced([near_hidden], [CAP * len(NEAR) * members])
    slots = [(s, i) for s in groups for i in range(len(NEAR))]
    starts = [[(s * len(NEAR) + i) * CAP] * len(near_terms) for s, i in slots]
    for (s, i), total in zip(slots, add_rows(near_terms, starts)):
        d = NEAR[i]
        if s or d:
            total = send(total, lambda e, m, t, d=d, s=s: (e ^ d, (m + members - s) % members, t))
        pieces[d].append(total)
    picks, weights = plan(members, routes_t, weight_t)
    owners = [d for d in range(EXPERTS) for _ in pieces[d][:1]]
    early = gather(picks, owners, [pieces[d][0] for d in owners])
    owners = [d for d in range(EXPERTS) for _ in pieces[d][1:]]
    return mix(weights, picks, early, owners, [x for d in range(EXPERTS) for x in pieces[d][1:]])


def solution(mesh):
    members = mesh.shape["ep"] // EXPERTS
    parts = mesh.shape["tp"]
    rows = P(("rep", "ep"), None)
    columns = P(None, ("ep", "tp"))
    placed = (rows, rows, rows, columns, columns, columns, columns, P(("ep", "tp"), None), P(("ep", "tp"), None))

    def body(*args):
        return layer(members, parts, *args)

    return jax.shard_map(
        body, mesh=mesh, in_specs=placed, out_specs=P(("rep", "ep"), "tp"), check_vma=False
    )
```
